32 devices in a mesh: ent: 16 (over z, y, x), dim: 2 (over core).
Axes of the slice: x: 2, y: 2, z: 4, core: 2. Of those that a mesh axis runs over, the one named last changes fastest.
Arguments:
- entities: float32 [32768, 1024], P('ent', 'dim'), may hold values from -3 to 3
- ent_state: float32 [32768], P('ent'), may hold values from 0.01 to 0.1
- buckets: int32 [32768], P('ent'), may hold values from 0 to 7
- relations: float32 [4096, 1024], P(None, 'dim'), may hold values from -1.6 to 1.6
- rel_state: float32 [4096], replicated, may hold values from 0.05 to 0.5
- triples: int32 [3, 8192], P(None, 'ent'), may hold values from 0 to 32767, as said below
- negatives: int32 [32, 256], P('ent'), may hold values from 0 to 32767, as said below
Outputs:
- new_entities: float32 [32768, 1024], P('ent', 'dim')
- new_relations: float32 [4096, 1024], P(None, 'dim')
The draws below stay inside these ranges and needn't reach their ends.
Inputs may be any that keep to these rules, and one draw needn't show every extreme that they name: `triples`: rows 0 and 2 hold entity ids, row 1 relation ids below 4096. The block of an entity id is id // 2048. Among the 768 ids of one group (its heads, its tails and its negatives) at most 128 lie in one block, and in every draw, for each rank of a group among the 2 groups of an index of ent, some block holds exactly 128 ids of that group on every index of ent. `negatives`: entity ids; they count in the bound on the ids of a group stated for triples.
All inputs are finite; a program needn't handle non-finite values.
Results may differ from the reference program's by a relative error of at most 0.0017.
Values may be sent and summed in bfloat16 or wider, within the bound.
A program may use at most 128 MiB of HBM per device.

```python
import math
import jax
import jax.numpy as jnp
from jax import lax

RANK = 512
BLK = 64
NREL = 4096
NEG = 256
GROUP = 256
NBUCK = 8
GROUP_DEV = 2
ENT_DEV = 2048
NENT = 32768
GROUPS = 32
TRIPLES = 8192
REQC = 768
CAPC = 128


def group_entity_ids(key):
    owner_count = NENT // ENT_DEV
    labels = jnp.repeat(jnp.arange(owner_count, dtype=jnp.int32), CAPC)
    star_owner = jax.random.randint(jax.random.fold_in(key, 11), (GROUP_DEV,), 0, owner_count)

    def one_group(group_key, full_owner):
        first_key, second_key, third_key, fourth_key = jax.random.split(group_key, 4)
        scores = jax.random.permutation(first_key, owner_count * CAPC).astype(jnp.int32)
        scores = jnp.where(labels == full_owner, scores - owner_count * CAPC, scores)
        order = jnp.argsort(scores, stable=True)
        chosen = labels[order[:REQC]]
        chosen = chosen[jax.random.permutation(second_key, REQC)]
        upper = jax.random.randint(third_key, (REQC,), 1, ENT_DEV + 1)
        local_rows = jax.random.randint(fourth_key, (REQC,), 0, upper)
        return chosen * ENT_DEV + local_rows
    group_keys = jax.random.split(jax.random.fold_in(key, 7), GROUPS)
    full_owners = star_owner[jnp.arange(GROUPS) % GROUP_DEV]
    return jax.vmap(one_group)(group_keys, full_owners).astype(jnp.int32)


def draw_triples(key, part):
    entity_ids = group_entity_ids(key)
    head_ids = entity_ids[:, :GROUP].reshape(TRIPLES)
    tail_ids = entity_ids[:, GROUP:2 * GROUP].reshape(TRIPLES)
    upper = jax.random.randint(jax.random.fold_in(key, 13), (TRIPLES,), 1, NREL + 1)
    rel_ids = jax.random.randint(jax.random.fold_in(key, 17), (TRIPLES,), 0, upper)
    return jnp.stack([head_ids, rel_ids.astype(jnp.int32), tail_ids], axis=0)


def draw_negatives(key, part):
    entity_ids = group_entity_ids(key)
    return entity_ids[:, 2 * GROUP:]


def touch_ends(values, own_key, smallest, high):
    spot = [jax.random.randint(jax.random.fold_in(own_key, axis), (), 0, length) for axis, length in enumerate(values.shape)]
    main_axis = values.shape.index(max(values.shape))
    next_to = spot[:main_axis] + [(spot[main_axis] + 1) % values.shape[main_axis]] + spot[main_axis + 1:]
    return values.at[tuple(spot)].set(smallest).at[tuple(next_to)].set(high)


def shard_levels(stream_key, extent, pieces, smallest, high):
    def one(position, blocks):
        heights = jax.random.uniform(jax.random.fold_in(jax.random.fold_in(stream_key, 6), position), (blocks,), jnp.float32, smallest / len(pieces), high / len(pieces))
        return jnp.repeat(jnp.exp(heights), extent[position] // blocks).reshape((-1,) + (1,) * (len(extent) - position - 1))

    gain = one(*pieces[0])
    for cut in pieces[1:]:
        gain = gain * one(*cut)
    return gain


def noise(key, shape, scale, bound, pieces=(), kind=jnp.bfloat16):
    array = jax.random.normal(key, shape, jnp.float32) * scale
    if len(pieces) > 0:
        array = shard_levels(key, shape, pieces, -0.22, 0.18) * array
    return jnp.clip(array, min=-bound, max=bound).astype(kind)


def setup_inputs(seed: int = 0) -> dict:
    splits = jax.random.split(jax.random.key(seed), 8)
    entities = noise(splits[0], (NENT, 2 * RANK), 0.5, 3.0, ((0, 16), (1, 2)), jnp.float32)
    ent_state = jnp.clip(jnp.exp(math.log(0.1) - 2.3025851 * jax.random.uniform(splits[1], (NENT,), jnp.float32) ** shard_levels(splits[1], (NENT,), ((0, 16),), -0.2, 0.2)), 0.01, 0.1)
    buckets = touch_ends(jax.random.randint(splits[2], (NENT,), 0, NBUCK), jax.random.fold_in(splits[2], 1), 0, NBUCK - 1).astype(jnp.int32)
    relations = noise(splits[3], (NREL, 2 * RANK), 0.27, 1.6, ((1, 2),), jnp.float32)
    rel_state = jnp.clip(jnp.exp(jax.random.uniform(splits[4], (NREL,), jnp.float32, math.log(0.05), math.log(0.5))), 0.05, 0.5)
    triples = draw_triples(jax.random.fold_in(splits[7], 71), 0)
    negatives = draw_negatives(jax.random.fold_in(splits[7], 71), 0)
    return {"entities": entities, "ent_state": ent_state, "buckets": buckets, "relations": relations, "rel_state": rel_state, "triples": triples, "negatives": negatives}


LEARN_RATE = 0.1
REG_WEIGHT = 0.01

def halves(values):
    shaped = values.reshape(values.shape[:-1] + (values.shape[-1] // (2 * BLK), 2, BLK))
    return (shaped[..., 0, :], shaped[..., 1, :])

def joined(real_part, imag_part):
    stacked = jnp.stack([real_part, imag_part], axis=-2)
    return stacked.reshape(stacked.shape[:-3] + (stacked.shape[-3] * 2 * BLK,))

def complex_product(former, latter):
    former_re, former_im = halves(former)
    latter_re, latter_im = halves(latter)
    return joined(former_re * latter_re - former_im * latter_im, former_re * latter_im + former_im * latter_re)

def conjugate(values):
    real_part, imag_part = halves(values)
    return joined(real_part, -imag_part)

def rounded_back(values):
    return lax.optimization_barrier(values.astype(jnp.bfloat16)).astype(jnp.float32)

def adagrad(table, state, grad):
    new_state = state + lax.optimization_barrier(jnp.mean(grad * grad, axis=-1))
    return table - LEARN_RATE * grad / jnp.sqrt(new_state)[:, None]

def reference(entities, ent_state, buckets, relations, rel_state, triples, negatives):
    ent_low = lax.optimization_barrier(entities.astype(jnp.bfloat16))
    rel_low = lax.optimization_barrier(relations.astype(jnp.bfloat16))
    head_ids = triples[0]
    rel_ids = triples[1]
    tail_ids = triples[2]
    head_rows = ent_low[head_ids].astype(jnp.float32)
    tail_rows = ent_low[tail_ids].astype(jnp.float32)
    rel_rows = rel_low[rel_ids].astype(jnp.float32)
    noise_rows = ent_low[negatives].astype(jnp.float32)
    query = rounded_back(complex_product(head_rows, rel_rows))
    probe = rounded_back(complex_product(conjugate(rel_rows), tail_rows))
    pos_score = lax.optimization_barrier(jnp.sum(query * tail_rows, axis=-1))
    query_groups = query.reshape(GROUPS, GROUP, 2 * RANK)
    probe_groups = probe.reshape(GROUPS, GROUP, 2 * RANK)
    tail_score = jnp.einsum('cid,cnd->cin', query_groups, noise_rows)
    head_score = jnp.einsum('cid,cnd->cin', probe_groups, noise_rows)
    pos_coef = rounded_back(-jax.nn.sigmoid(-pos_score))
    tail_coef = rounded_back(jax.nn.sigmoid(tail_score) / NEG)
    head_coef = rounded_back(jax.nn.sigmoid(head_score) / NEG)
    tail_pull = pos_coef[:, None] * tail_rows + jnp.einsum('cin,cnd->cid', tail_coef, noise_rows).reshape(TRIPLES, 2 * RANK)
    head_pull = jnp.einsum('cin,cnd->cid', head_coef, noise_rows).reshape(TRIPLES, 2 * RANK)
    head_side = pos_coef[:, None] * head_rows + head_pull
    head_grad = complex_product(conjugate(rel_rows), tail_pull).astype(jnp.bfloat16)
    tail_grad = complex_product(rel_rows, head_side).astype(jnp.bfloat16)
    noise_grad = (jnp.einsum('cin,cid->cnd', tail_coef, query_groups) + jnp.einsum('cin,cid->cnd', head_coef, probe_groups)).astype(jnp.bfloat16)
    rel_grad_rows = complex_product(conjugate(head_rows), tail_pull) + complex_product(tail_rows, conjugate(head_pull))
    all_ids = jnp.concatenate([head_ids, tail_ids, negatives.reshape(-1)]).astype(jnp.int32)
    all_grads = jnp.concatenate([head_grad, tail_grad, noise_grad.reshape(GROUPS * NEG, 2 * RANK)], axis=0).astype(jnp.float32)
    ent_grad = jnp.zeros((NENT, 2 * RANK), jnp.float32).at[all_ids].add(all_grads)
    counts = jnp.zeros((NENT,), jnp.float32).at[all_ids].add(jnp.ones(all_ids.shape, jnp.float32))
    weight = REG_WEIGHT * (buckets.astype(jnp.float32) + 1.0) * counts
    ent_grad = ent_grad + weight[:, None] * 3.0 * entities * jnp.abs(entities)
    rel_grad = jnp.zeros((NREL, 2 * RANK), jnp.float32).at[rel_ids].add(rel_grad_rows)
    return (adagrad(entities, ent_state, ent_grad), adagrad(relations, rel_state, rel_grad))
```

```python
import jax
import jax.numpy as jnp
from jax import lax
from jax.sharding import PartitionSpec as P

RANK = 512
BLK = 64


LEARN_RATE = 0.1
REG_WEIGHT = 0.01


def halves(values):
    shaped = values.reshape(values.shape[:-1] + (values.shape[-1] // (2 * BLK), 2, BLK))
    return (shaped[..., 0, :], shaped[..., 1, :])


def joined(real_part, imag_part):
    stacked = jnp.stack([real_part, imag_part], axis=-2)
    return stacked.reshape(stacked.shape[:-3] + (stacked.shape[-3] * 2 * BLK,))


def complex_product(former, latter):
    former_re, former_im = halves(former)
    latter_re, latter_im = halves(latter)
    return joined(
        former_re * latter_re - former_im * latter_im, former_re * latter_im + former_im * latter_re
    )


def conjugate(values):
    real_part, imag_part = halves(values)
    return joined(real_part, -imag_part)


def rounded(values):
    return lax.optimization_barrier(values.astype(jnp.bfloat16))


def contract_first(former, latter):
    return lax.dot_general(
        former, latter, (((0,), (0,)), ((), ())), preferred_element_type=jnp.float32
    )


def contract_last(former, latter):
    return lax.dot_general(
        former, latter, (((1,), (1,)), ((), ())), preferred_element_type=jnp.float32
    )


def exchange(blocks):
    return [
        lax.all_to_all(block, "ent", split_axis=0, concat_axis=0, tiled=True) for block in blocks
    ]


def group_step(rows_group, rel_float, group_len):
    head_float = rows_group[:group_len].astype(jnp.float32)
    tail_float = rows_group[group_len : 2 * group_len].astype(jnp.float32)
    noise_rows = rows_group[2 * group_len :]
    width_neg = noise_rows.shape[0]
    query = rounded(complex_product(head_float, rel_float))
    probe = rounded(complex_product(conjugate(rel_float), tail_float))
    part_pos = jnp.sum(query.astype(jnp.float32) * tail_float, axis=-1, keepdims=True)
    part = jnp.concatenate(
        [
            contract_last(query, noise_rows),
            contract_last(probe, noise_rows),
            jnp.broadcast_to(part_pos, (group_len, 128)),
        ],
        axis=1,
    ).astype(jnp.bfloat16)
    scores = jnp.sum(lax.all_gather(part, "dim").astype(jnp.float32), axis=0)
    both_coef = rounded(jax.nn.sigmoid(scores[:, : 2 * width_neg]) / width_neg)
    pos_float = -jax.nn.sigmoid(-scores[:, 2 * width_neg : 2 * width_neg + 1])
    pos_float = rounded(pos_float).astype(jnp.float32)
    tail_coef = both_coef[:, :width_neg]
    head_coef = both_coef[:, width_neg:]
    tail_pull = pos_float * tail_float + jnp.dot(
        tail_coef, noise_rows, preferred_element_type=jnp.float32
    )
    head_pull = jnp.dot(head_coef, noise_rows, preferred_element_type=jnp.float32)
    head_side = pos_float * head_float + head_pull
    head_grad = complex_product(conjugate(rel_float), tail_pull).astype(jnp.bfloat16)
    tail_grad = complex_product(rel_float, head_side).astype(jnp.bfloat16)
    noise_grad = (contract_first(tail_coef, query) + contract_first(head_coef, probe)).astype(
        jnp.bfloat16
    )
    rel_grad = complex_product(conjugate(head_float), tail_pull) + complex_product(
        tail_float, conjugate(head_pull)
    )
    return (
        jnp.concatenate([head_grad, tail_grad, noise_grad], axis=0),
        rel_grad.astype(jnp.bfloat16),
    )


def placement_of(wanted_row, owners, rows_here, slot_count):
    request_count = wanted_row.shape[0]
    owner_of = wanted_row // rows_here
    owner_hits = (owner_of[:, None] == jnp.arange(owners, dtype=jnp.int32)[None, :]).astype(
        jnp.bfloat16
    )
    order = jnp.arange(request_count, dtype=jnp.int32)
    earlier = (order[:, None] > order[None, :]).astype(jnp.bfloat16)
    before = jnp.dot(earlier, owner_hits, preferred_element_type=jnp.float32)
    slot_rank = jnp.sum(before * owner_hits.astype(jnp.float32), axis=-1).astype(jnp.int32)
    slot_flat = owner_of * slot_count + slot_rank
    matches = slot_flat[:, None] == jnp.arange(owners * slot_count, dtype=jnp.int32)[None, :]
    slot_ids = jnp.sum(jnp.where(matches, wanted_row[:, None] + 1, 0), axis=0) - 1
    return (matches.astype(jnp.bfloat16), slot_ids.reshape(owners, slot_count))


def accumulate(local_rows, received_rows, totals, counts):
    flat_rows = received_rows.reshape(local_rows.shape[0], received_rows.shape[-1])
    positions = jnp.arange(totals.shape[0], dtype=jnp.int32)
    one_hot = (local_rows[:, None] == positions[None, :]).astype(jnp.bfloat16)
    totals = totals + contract_first(one_hot, flat_rows)
    counts = counts + jnp.sum(one_hot, axis=0, dtype=jnp.float32)
    return (totals, counts)


def adagrad(table, state, grad, squares):
    new_state = state + squares / (2 * RANK)
    scale = LEARN_RATE / jnp.sqrt(new_state)
    return table - grad * scale[:, None]


def per_device(entities, ent_state, buckets, relations, rel_state, triples, negatives):
    owners = lax.axis_size("ent")
    rows_here, columns_here = entities.shape
    rel_count = relations.shape[0]
    row_base = lax.axis_index("ent") * rows_here
    groups_here = negatives.shape[0]
    group_len = triples.shape[1] // groups_here
    request_count = 2 * group_len + negatives.shape[1]
    slot_count = 8 * ((request_count + 3 * owners - 1) // (3 * owners))
    ent_low = entities.astype(jnp.bfloat16)
    head_ids = triples[0].reshape(groups_here, group_len)
    tail_ids = triples[2].reshape(groups_here, group_len)
    wanted = jnp.concatenate([head_ids, tail_ids, negatives], axis=1)
    placed = [
        placement_of(wanted[index], owners, rows_here, slot_count) for index in range(groups_here)
    ]
    slot_ids = jnp.stack([slots for _, slots in placed], axis=1)
    received = lax.all_to_all(slot_ids, "ent", split_axis=0, concat_axis=0, tiled=True)
    local_rows = [received[:, index].reshape(-1) - row_base for index in range(groups_here)]
    looked_up = [
        jnp.take(ent_low, jnp.clip(rows, 0, rows_here - 1), axis=0).reshape(
            owners, slot_count, columns_here
        )
        for rows in local_rows
    ]
    arrived = exchange(looked_up)
    rel_float = rounded(jnp.take(relations, triples[1], axis=0)).astype(jnp.float32)
    outgoing, rel_rows = [], []
    for index in range(groups_here):
        matches = placed[index][0]
        rows_group = jnp.dot(
            matches,
            arrived[index].reshape(owners * slot_count, columns_here),
            preferred_element_type=jnp.float32,
        ).astype(jnp.bfloat16)
        grads, rel_row = group_step(
            rows_group, rel_float[index * group_len : (index + 1) * group_len], group_len
        )
        outgoing.append(
            contract_first(matches, grads)
            .astype(jnp.bfloat16)
            .reshape(owners, slot_count, columns_here)
        )
        rel_rows.append(rel_row)
    rel_hits = (
        triples[1][:, None] == jnp.arange(rel_count, dtype=jnp.int32)[None, :]
    ).astype(jnp.bfloat16)
    rel_part = contract_first(rel_hits, jnp.concatenate(rel_rows, axis=0)).astype(jnp.bfloat16)
    rel_share = lax.psum_scatter(rel_part, "ent", scatter_dimension=0, tiled=True)
    rel_grad = lax.all_gather(rel_share, "ent", axis=0, tiled=True).astype(jnp.float32)
    returned = exchange(outgoing)
    totals = jnp.zeros((rows_here, columns_here), jnp.float32)
    counts = jnp.zeros((rows_here,), jnp.float32)
    for index in range(groups_here):
        totals, counts = accumulate(local_rows[index], returned[index], totals, counts)
    weight = REG_WEIGHT * (buckets.astype(jnp.float32) + 1.0) * counts
    totals = totals + weight[:, None] * 3.0 * entities * jnp.abs(entities)
    ent_squares = jnp.sum(totals * totals, axis=-1)
    ent_all, rel_all = lax.psum((ent_squares, jnp.sum(rel_grad * rel_grad, axis=-1)), "dim")
    new_relations = adagrad(relations, rel_state, rel_grad, rel_all)
    new_entities = adagrad(entities, ent_state, totals, ent_all)
    return (new_entities, new_relations)


def solution(mesh):
    placed = (
        P("ent", "dim"),
        P("ent"),
        P("ent"),
        P(None, "dim"),
        P(),
        P(None, "ent"),
        P("ent", None),
    )
    return jax.shard_map(
        per_device,
        mesh=mesh,
        in_specs=placed,
        out_specs=(P("ent", "dim"), P(None, "dim")),
        check_vma=False,
    )
```

```python
import jax
import jax.numpy as jnp
from jax import lax
from jax.sharding import PartitionSpec as P

RANK = 512
BLK = 64


LEARN_RATE = 0.1
REG_WEIGHT = 0.01


def halves(values):
    shaped = values.reshape(values.shape[:-1] + (values.shape[-1] // (2 * BLK), 2, BLK))
    return (shaped[..., 0, :], shaped[..., 1, :])


def joined(real_part, imag_part):
    stacked = jnp.stack([real_part, imag_part], axis=-2)
    return stacked.reshape(stacked.shape[:-3] + (stacked.shape[-3] * 2 * BLK,))


def complex_product(former, latter):
    former_re, former_im = halves(former)
    latter_re, latter_im = halves(latter)
    return joined(
        former_re * latter_re - former_im * latter_im, former_re * latter_im + former_im * latter_re
    )


def conjugate(values):
    real_part, imag_part = halves(values)
    return joined(real_part, -imag_part)


def rounded(values):
    return lax.optimization_barrier(values.astype(jnp.bfloat16))


def contract_first(former, latter):
    return lax.dot_general(
        former, latter, (((0,), (0,)), ((), ())), preferred_element_type=jnp.float32
    )


def contract_last(former, latter):
    return lax.dot_general(
        former, latter, (((1,), (1,)), ((), ())), preferred_element_type=jnp.float32
    )


def exchange(blocks):
    return [
        lax.all_to_all(block, "ent", split_axis=0, concat_axis=0, tiled=True) for block in blocks
    ]


def group_step(rows_group, rel_float, group_len):
    head_float = rows_group[:group_len].astype(jnp.float32)
    tail_float = rows_group[group_len : 2 * group_len].astype(jnp.float32)
    noise_rows = rows_group[2 * group_len :]
    width_neg = noise_rows.shape[0]
    query = rounded(complex_product(head_float, rel_float))
    probe = rounded(complex_product(conjugate(rel_float), tail_float))
    part_pos = jnp.sum(query.astype(jnp.float32) * tail_float, axis=-1, keepdims=True)
    part = jnp.concatenate(
        [
            contract_last(query, noise_rows),
            contract_last(probe, noise_rows),
            jnp.broadcast_to(part_pos, (group_len, 128)),
        ],
        axis=1,
    ).astype(jnp.bfloat16)
    scores = jnp.sum(lax.all_gather(part, "dim").astype(jnp.float32), axis=0)
    both_coef = rounded(jax.nn.sigmoid(scores[:, : 2 * width_neg]) / width_neg)
    pos_float = -jax.nn.sigmoid(-scores[:, 2 * width_neg : 2 * width_neg + 1])
    pos_float = rounded(pos_float).astype(jnp.float32)
    tail_coef = both_coef[:, :width_neg]
    head_coef = both_coef[:, width_neg:]
    tail_pull = pos_float * tail_float + jnp.dot(
        tail_coef, noise_rows, preferred_element_type=jnp.float32
    )
    head_pull = jnp.dot(head_coef, noise_rows, preferred_element_type=jnp.float32)
    head_side = pos_float * head_float + head_pull
    head_grad = complex_product(conjugate(rel_float), tail_pull).astype(jnp.bfloat16)
    tail_grad = complex_product(rel_float, head_side).astype(jnp.bfloat16)
    noise_grad = (contract_first(tail_coef, query) + contract_first(head_coef, probe)).astype(
        jnp.bfloat16
    )
    rel_grad = complex_product(conjugate(head_float), tail_pull) + complex_product(
        tail_float, conjugate(head_pull)
    )
    return (
        jnp.concatenate([head_grad, tail_grad, noise_grad], axis=0),
        rel_grad.astype(jnp.bfloat16),
    )


def placement_of(wanted_row, owners, rows_here, slot_count):
    request_count = wanted_row.shape[0]
    owner_of = wanted_row // rows_here
    owner_hits = (owner_of[:, None] == jnp.arange(owners, dtype=jnp.int32)[None, :]).astype(
        jnp.bfloat16
    )
    order = jnp.arange(request_count, dtype=jnp.int32)
    earlier = (order[:, None] > order[None, :]).astype(jnp.bfloat16)
    before = jnp.dot(earlier, owner_hits, preferred_element_type=jnp.float32)
    slot_rank = jnp.sum(before * owner_hits.astype(jnp.float32), axis=-1).astype(jnp.int32)
    slot_flat = owner_of * slot_count + slot_rank
    matches = slot_flat[:, None] == jnp.arange(owners * slot_count, dtype=jnp.int32)[None, :]
    slot_ids = jnp.sum(jnp.where(matches, wanted_row[:, None] + 1, 0), axis=0) - 1
    return (matches.astype(jnp.bfloat16), slot_ids.reshape(owners, slot_count))


def accumulate(local_rows, received_rows, totals, counts):
    flat_rows = received_rows.reshape(local_rows.shape[0], received_rows.shape[-1])
    positions = jnp.arange(totals.shape[0], dtype=jnp.int32)
    one_hot = (local_rows[:, None] == positions[None, :]).astype(jnp.bfloat16)
    totals = totals + contract_first(one_hot, flat_rows)
    counts = counts + jnp.sum(one_hot, axis=0, dtype=jnp.float32)
    return (totals, counts)


def teams(owners):
    near_size = 4 if owners % 4 == 0 else 1
    far_size = owners // near_size
    near = [[row * near_size + place for place in range(near_size)] for row in range(far_size)]
    far = [[row * near_size + place for row in range(far_size)] for place in range(near_size)]
    return (near, far)


def sum_relations(rel_rows, near_ids, rel_count, near, far):
    near_size, far_size = len(far), len(near)
    row_count, columns = rel_rows.shape
    tiles = rel_rows.reshape(row_count, near_size, columns // near_size).transpose(1, 0, 2)
    tiles = lax.all_to_all(
        tiles, "ent", split_axis=0, concat_axis=0, axis_index_groups=near, tiled=True
    )
    hits = (near_ids[:, None] == jnp.arange(rel_count, dtype=jnp.int32)[None, :]).astype(
        jnp.bfloat16
    )
    part = contract_first(hits, tiles.reshape(near_size * row_count, columns // near_size)).astype(
        jnp.bfloat16
    )
    share = lax.psum_scatter(
        part, "ent", scatter_dimension=0, axis_index_groups=far, tiled=True
    )
    whole = lax.all_gather(share, "ent", axis=0)
    whole = whole.reshape(far_size, near_size, rel_count // far_size, columns // near_size)
    return whole.transpose(0, 2, 1, 3).reshape(rel_count, columns).astype(jnp.float32)


def adagrad(table, state, grad, squares):
    new_state = state + squares / (2 * RANK)
    scale = LEARN_RATE / jnp.sqrt(new_state)
    return table - grad * scale[:, None]


def per_device(entities, ent_state, buckets, relations, rel_state, triples, negatives):
    owners = lax.axis_size("ent")
    rows_here, columns_here = entities.shape
    rel_count = relations.shape[0]
    row_base = lax.axis_index("ent") * rows_here
    groups_here = negatives.shape[0]
    group_len = triples.shape[1] // groups_here
    request_count = 2 * group_len + negatives.shape[1]
    slot_count = 8 * ((request_count + 3 * owners - 1) // (3 * owners))
    ent_low = entities.astype(jnp.bfloat16)
    head_ids = triples[0].reshape(groups_here, group_len)
    tail_ids = triples[2].reshape(groups_here, group_len)
    wanted = jnp.concatenate([head_ids, tail_ids, negatives], axis=1)
    placed = [
        placement_of(wanted[index], owners, rows_here, slot_count) for index in range(groups_here)
    ]
    near, far = teams(owners)
    near_ids = lax.all_gather(triples[1], "ent", axis_index_groups=near, tiled=True)
    slot_ids = jnp.stack([slots for _, slots in placed], axis=1)
    received = lax.all_to_all(slot_ids, "ent", split_axis=0, concat_axis=0, tiled=True)
    local_rows = [received[:, index].reshape(-1) - row_base for index in range(groups_here)]
    looked_up = [
        jnp.take(ent_low, rows, axis=0, mode="clip").reshape(
            owners, slot_count, columns_here
        )
        for rows in local_rows
    ]
    arrived = exchange(looked_up)
    rel_float = rounded(jnp.take(relations, triples[1], axis=0, mode="clip")).astype(jnp.float32)
    outgoing, rel_rows = [], []
    for index in range(groups_here):
        matches = placed[index][0]
        rows_group = jnp.dot(
            matches,
            arrived[index].reshape(owners * slot_count, columns_here),
            preferred_element_type=jnp.float32,
        ).astype(jnp.bfloat16)
        grads, rel_row = group_step(
            rows_group, rel_float[index * group_len : (index + 1) * group_len], group_len
        )
        sent = (
            contract_first(matches, grads)
            .astype(jnp.bfloat16)
            .reshape(owners, slot_count, columns_here)
        )
        if index + 1 < groups_here:
            sent, arrived[index + 1] = lax.optimization_barrier((sent, arrived[index + 1]))
        outgoing.append(sent)
        rel_rows.append(rel_row)
    rel_grad = sum_relations(jnp.concatenate(rel_rows, axis=0), near_ids, rel_count, near, far)
    returned = exchange(outgoing)
    totals = jnp.zeros((rows_here, columns_here), jnp.float32)
    counts = jnp.zeros((rows_here,), jnp.float32)
    for index in range(groups_here):
        totals, counts = accumulate(local_rows[index], returned[index], totals, counts)
    weight = REG_WEIGHT * (buckets.astype(jnp.float32) + 1.0) * counts
    totals = totals + weight[:, None] * 3.0 * entities * jnp.abs(entities)
    ent_squares = jnp.sum(totals * totals, axis=-1)
    ent_all, rel_all = lax.psum((ent_squares, jnp.sum(rel_grad * rel_grad, axis=-1)), "dim")
    new_relations = adagrad(relations, rel_state, rel_grad, rel_all)
    new_entities = adagrad(entities, ent_state, totals, ent_all)
    return (new_entities, new_relations)


def solution(mesh):
    placed = (
        P("ent", "dim"),
        P("ent"),
        P("ent"),
        P(None, "dim"),
        P(),
        P(None, "ent"),
        P("ent", None),
    )
    return jax.shard_map(
        per_device,
        mesh=mesh,
        in_specs=placed,
        out_specs=(P("ent", "dim"), P(None, "dim")),
        check_vma=False,
    )
```
